8 devices in a mesh: stage: 2 (over z, y), data: 4 (over x, core).
Axes of the slice: x: 2, y: 2, z: 1, core: 2. Of those that a mesh axis runs over, the one named last changes fastest.
Arguments:
- x_in: bfloat16 [24, 8192, 256], P(None, 'data')
- targets: bfloat16 [24, 8192, 256], P(None, 'data')
- w1_bf: bfloat16 [2, 2, 2, 256, 1024], P('stage')
- w2_bf: bfloat16 [2, 2, 2, 1024, 256], P('stage')
- w_master: float32 [2, 2, 2, 524288], P('stage', None, None, 'data')
- m_state: float32 [2, 2, 2, 524288], P('stage', None, None, 'data')
- v_state: float32 [2, 2, 2, 524288], P('stage', None, None, 'data')
Outputs:
- output 1: bfloat16 [2, 2, 2, 256, 1024], P('stage')
- output 2: bfloat16 [2, 2, 2, 1024, 256], P('stage')
- output 3: float32 [2, 2, 2, 524288], P('stage', None, None, 'data')
- output 4: float32 [2, 2, 2, 524288], P('stage', None, None, 'data')
- output 5: float32 [2, 2, 2, 524288], P('stage', None, None, 'data')
- output 6: float32 [], replicated
All inputs are finite; a program needn't handle non-finite values.
Results may differ from the reference program's by a relative error of at most 0.001.
Values are sent between devices in bfloat16 or wider.
A program may use at most 1 GiB of HBM per device.

```python
import math
import jax
import jax.numpy as jnp
from jax import lax

STAGES = 2
DATA_WAYS = 4
MB_GROUPS = 12
TOK_DEV = 2048
VSTAGE_BLOCKS = 2
D_MODEL = 256
ADAM_STEP = 1000

N_MICRO = MB_GROUPS * STAGES
N_ROWS = DATA_WAYS * TOK_DEV
D_FF = 4 * D_MODEL
N_BLOCKS = 2 * STAGES * VSTAGE_BLOCKS
N_TOKENS = N_MICRO * N_ROWS
FLAT_LEN = 8 * D_MODEL * D_MODEL
N_PARAMS = N_BLOCKS * FLAT_LEN
BETA_ONE = 0.9
BETA_TWO = 0.999
ADAM_EPS = 1e-8
WEIGHT_DECAY = 0.1
TAU_CLIP = 0.3 * D_MODEL * math.sqrt(N_BLOCKS * (3.0 / N_TOKENS + 0.008))
LEARN_RATE = 0.1 / math.sqrt(4.0 * D_MODEL * N_BLOCKS)


def gelu_tanh(pre_act):
    return jax.nn.gelu(pre_act, approximate=True)


def moment_scale():
    scale_two = TAU_CLIP * math.sqrt(2.0 / (N_PARAMS * (1.0 + 1.0 / N_BLOCKS)))
    scale_one = scale_two / math.sqrt(N_BLOCKS)
    return jnp.concatenate([jnp.full((D_MODEL * D_FF,), scale_one, jnp.float32), jnp.full((D_FF * D_MODEL,), scale_two, jnp.float32)])


def setup_inputs(seed: int = 0) -> dict:
    key_list = jax.random.split(jax.random.key(seed), 6)
    act_shape = (N_MICRO, N_ROWS, D_MODEL)
    lead_dims = (STAGES, 2, VSTAGE_BLOCKS)
    x_in = jax.random.normal(key_list[0], act_shape, jnp.float32)
    targets = jax.random.normal(key_list[1], act_shape, jnp.float32)
    w_one = jax.random.normal(key_list[2], lead_dims + (D_MODEL, D_FF), jnp.float32) * D_MODEL ** -0.5
    w_two = jax.random.normal(key_list[3], lead_dims + (D_FF, D_MODEL), jnp.float32) * (D_FF * N_BLOCKS) ** -0.5
    w_master = jnp.concatenate([w_one.reshape(lead_dims + (-1,)), w_two.reshape(lead_dims + (-1,))], axis=-1)
    elem_scale = moment_scale()
    m_state = 0.5 * elem_scale * jax.random.normal(key_list[4], w_master.shape, jnp.float32)
    v_state = elem_scale * elem_scale * (0.25 + 0.5 * jax.random.uniform(key_list[5], w_master.shape, jnp.float32))
    return dict(x_in=x_in.astype(jnp.bfloat16), targets=targets.astype(jnp.bfloat16), w1_bf=w_one.astype(jnp.bfloat16), w2_bf=w_two.astype(jnp.bfloat16), w_master=w_master, m_state=m_state, v_state=v_state)


def block_forward(h_in, w_one, w_two):
    pre_act = jnp.dot(h_in, w_one, preferred_element_type=jnp.float32)
    act_bf = gelu_tanh(pre_act).astype(jnp.bfloat16)
    out_val = h_in.astype(jnp.float32) + jnp.dot(act_bf, w_two, preferred_element_type=jnp.float32)
    return out_val.astype(jnp.bfloat16)


def block_backward(h_in, grad_out, w_one, w_two):
    pre_act = jnp.dot(h_in, w_one, preferred_element_type=jnp.float32)
    act_val, gelu_pull = jax.vjp(gelu_tanh, pre_act)
    act_bf = act_val.astype(jnp.bfloat16)
    grad_act = jnp.dot(grad_out, w_two.T, preferred_element_type=jnp.float32)
    grad_pre = gelu_pull(grad_act)[0].astype(jnp.bfloat16)
    back_val = jnp.dot(grad_pre, w_one.T, preferred_element_type=jnp.float32)
    grad_in = (grad_out.astype(jnp.float32) + back_val).astype(jnp.bfloat16)
    grad_one = jnp.dot(h_in.T, grad_pre, preferred_element_type=jnp.float32)
    grad_two = jnp.dot(act_bf.T, grad_out, preferred_element_type=jnp.float32)
    return grad_in, grad_one, grad_two


def reference(x_in, targets, w1_bf, w2_bf, w_master, m_state, v_state):
    w_ones = jnp.swapaxes(w1_bf, 0, 1).reshape(N_BLOCKS, D_MODEL, D_FF)
    w_twos = jnp.swapaxes(w2_bf, 0, 1).reshape(N_BLOCKS, D_FF, D_MODEL)

    def fwd_step(h_in, weights):
        return block_forward(h_in, weights[0], weights[1]), h_in

    def bwd_step(grad_out, saved_item):
        grad_in, grad_one, grad_two = block_backward(saved_item[0], grad_out, saved_item[1], saved_item[2])
        return grad_in, (grad_one, grad_two)

    def micro_step(state_carry, mb_pair):
        acc_one, acc_two, loss_acc = state_carry
        h_out, block_inputs = lax.scan(fwd_step, mb_pair[0], (w_ones, w_twos))
        residual = h_out.astype(jnp.float32) - mb_pair[1].astype(jnp.float32)
        loss_acc = loss_acc + 0.5 * jnp.sum(residual * residual)
        grad_seed = (residual / N_TOKENS).astype(jnp.bfloat16)
        grad_pair = lax.scan(bwd_step, grad_seed, (block_inputs, w_ones, w_twos), reverse=True)[1]
        return (acc_one + grad_pair[0], acc_two + grad_pair[1], loss_acc), None

    start_carry = (jnp.zeros((N_BLOCKS, D_MODEL, D_FF), jnp.float32), jnp.zeros((N_BLOCKS, D_FF, D_MODEL), jnp.float32), jnp.zeros((), jnp.float32))
    acc_one, acc_two, loss_acc = lax.scan(micro_step, start_carry, (x_in, targets))[0]
    flat_dims = (2, STAGES, VSTAGE_BLOCKS, -1)
    grad_flat = jnp.swapaxes(jnp.concatenate([acc_one.reshape(flat_dims), acc_two.reshape(flat_dims)], axis=-1), 0, 1)
    grad_norm = jnp.sqrt(jnp.sum(grad_flat * grad_flat))
    clip_factor = jnp.minimum(1.0, TAU_CLIP / grad_norm)
    grad_clip = clip_factor * grad_flat
    m_new = BETA_ONE * m_state + (1.0 - BETA_ONE) * grad_clip
    v_new = BETA_TWO * v_state + (1.0 - BETA_TWO) * grad_clip * grad_clip
    m_hat = m_new / (1.0 - BETA_ONE ** ADAM_STEP)
    v_hat = v_new / (1.0 - BETA_TWO ** ADAM_STEP)
    w_new = w_master - LEARN_RATE * (m_hat / (jnp.sqrt(v_hat) + ADAM_EPS) + WEIGHT_DECAY * w_master)
    w_bf = w_new.astype(jnp.bfloat16)
    split_at = D_MODEL * D_FF
    w1_new = w_bf[..., :split_at].reshape(STAGES, 2, VSTAGE_BLOCKS, D_MODEL, D_FF)
    w2_new = w_bf[..., split_at:].reshape(STAGES, 2, VSTAGE_BLOCKS, D_FF, D_MODEL)
    return w1_new, w2_new, w_new, m_new, v_new, loss_acc / N_TOKENS
```

```python
import functools
import math
import jax
import jax.numpy as jnp
from jax import lax
from jax.experimental import pallas as pl
from jax.experimental.pallas import tpu as pltpu
from jax.sharding import PartitionSpec as P

BETA_ONE = 0.9
BETA_TWO = 0.999
ADAM_EPS = 1e-8
WEIGHT_DECAY = 0.1
ADAM_STEP = 1000

ROWS = 256
CHUNK = 256
SUB = 32
NBLK = 8
SQRT_2_PI = math.sqrt(2.0 / math.pi)
F32 = jnp.float32
BF16 = jnp.bfloat16


def block_slot(b):
    return ((b // 2) % 2) * 4 + (b // 4) * 2 + b % 2


def gelu_pair(u):
    u2 = u * u
    s = jax.nn.sigmoid(u * (u2 * (2.0 * SQRT_2_PI * 0.044715) + 2.0 * SQRT_2_PI))
    a = u * s
    w = u2 * (6.0 * SQRT_2_PI * 0.044715) + 2.0 * SQRT_2_PI
    return a, s + a * ((1.0 - s) * w)


def dot(a, b):
    return jnp.dot(a, b, preferred_element_type=F32)


def dot_t(a, b):
    return lax.dot_general(a, b, (((1,), (1,)), ((), ())), preferred_element_type=F32)


def step_kernel(n_tok_inv, off_ref, x_ref, t_ref, w1_ref, w2_ref, g1_ref, g2_ref, loss_ref,
                gp_ref, a_ref, h_ref, h_cur, seed_ref, loss_acc):
    i = pl.program_id(0)

    @pl.when(i == 0)
    def _():
        seed_ref[...] = jnp.zeros_like(seed_ref)

        def clear(b, _):
            for ref in (g1_ref, g2_ref):
                ref[b] = jnp.zeros(ref.shape[1:], ref.dtype)
            for ref in (gp_ref, a_ref, h_ref):
                ref[1, b] = jnp.zeros(ref.shape[2:], ref.dtype)
            return 0

        lax.fori_loop(0, NBLK, clear, 0)
        loss_acc[...] = jnp.zeros_like(loss_acc)

    for par in range(2):
        other = 1 - par
        rows_here = slice(par * ROWS, (par + 1) * ROWS)
        h_cur[...] = x_ref[rows_here, :]

        def body(j, _, par=par, other=other):
            bb = NBLK - 1 - j
            fs = lax.rem(lax.div(j, 2), 2) * 4 + lax.div(j, 4) * 2 + lax.rem(j, 2)
            bs = lax.rem(lax.div(bb, 2), 2) * 4 + lax.div(bb, 4) * 2 + lax.rem(bb, 2)
            h = h_cur[...]
            g = seed_ref[...]
            h_ref[par, j] = h
            h_t = h_ref[other, bb].T
            g_t = g.T
            h_acc = None
            g_acc = None
            for n in range(4):
                cols = slice(n * CHUNK, (n + 1) * CHUNK)
                q = dot_t(g, w2_ref[bs, cols, :])
                u = dot(h, w1_ref[fs, :, cols])
                rs = []
                for k in range(ROWS // SUB):
                    rr = slice(k * SUB, (k + 1) * SUB)
                    rs.append((q[rr] * gp_ref[other, bb, rr, cols]).astype(BF16))
                r = jnp.concatenate(rs, axis=0)
                al = []
                for k in range(ROWS // SUB):
                    rr = slice(k * SUB, (k + 1) * SUB)
                    av, gv = gelu_pair(u[rr])
                    gp_ref[par, j, rr, cols] = gv
                    al.append(av.astype(BF16))
                a = jnp.concatenate(al, axis=0)
                a_ref[par, j, :, cols] = a
                hp = dot(a, w2_ref[fs, cols, :])
                h_acc = hp if h_acc is None else h_acc + hp
                gpart = dot_t(r, w1_ref[bs, :, cols])
                g_acc = gpart if g_acc is None else g_acc + gpart
                g1_ref[bs, :, cols] += dot(h_t, r)
                g2_ref[bs, :, cols] += dot(g_t, a_ref[other, bb, :, cols])
            h_cur[...] = (h.astype(F32) + h_acc).astype(BF16)
            seed_ref[...] = (g.astype(F32) + g_acc).astype(BF16)
            return 0

        lax.fori_loop(0, NBLK, body, 0)
        res = h_cur[...].astype(F32) - t_ref[rows_here, :].astype(F32)
        res = jnp.where(i < pl.num_programs(0) - 1, res, 0.0)
        loss_acc[...] += jnp.sum((res * res).reshape(ROWS // 8, 8, 256), axis=0)
        seed_ref[...] = (res * n_tok_inv).astype(BF16)

    @pl.when(i == pl.num_programs(0) - 1)
    def _():
        loss_ref[...] = loss_acc[...]


def run_stack(x, t, w1, w2, off, n_rows, n_tokens):
    steps = n_rows // (2 * ROWS)
    row_map = lambda i, off: (off[0] + jnp.minimum(i, steps - 1), 0)
    const3 = lambda i, off: (0, 0, 0)
    spec = pltpu.PrefetchScalarGridSpec(
        num_scalar_prefetch=1,
        grid=(steps + 1,),
        in_specs=[
            pl.BlockSpec((2 * ROWS, 256), row_map),
            pl.BlockSpec((2 * ROWS, 256), row_map),
            pl.BlockSpec((NBLK, 256, 1024), const3, pipeline_mode=pl.Buffered(1)),
            pl.BlockSpec((NBLK, 1024, 256), const3, pipeline_mode=pl.Buffered(1)),
        ],
        out_specs=[
            pl.BlockSpec((NBLK, 256, 1024), const3, pipeline_mode=pl.Buffered(1)),
            pl.BlockSpec((NBLK, 256, 1024), const3, pipeline_mode=pl.Buffered(1)),
            pl.BlockSpec((8, 256), lambda i, off: (0, 0)),
        ],
        scratch_shapes=[
            pltpu.VMEM((2, NBLK, ROWS, 1024), F32),
            pltpu.VMEM((2, NBLK, ROWS, 1024), BF16),
            pltpu.VMEM((2, NBLK, ROWS, 256), BF16),
            pltpu.VMEM((ROWS, 256), BF16),
            pltpu.VMEM((ROWS, 256), BF16),
            pltpu.VMEM((8, 256), F32),
        ],
    )
    return pl.pallas_call(
        functools.partial(step_kernel, 1.0 / n_tokens),
        grid_spec=spec,
        out_shape=[
            jax.ShapeDtypeStruct((NBLK, 256, 1024), F32),
            jax.ShapeDtypeStruct((NBLK, 256, 1024), F32),
            jax.ShapeDtypeStruct((8, 256), F32),
        ],
        compiler_params=pltpu.CompilerParams(vmem_limit_bytes=67043328),
        name="stack_step",
    )(off, x, t, w1, w2)


def adam_update(w_old, m_old, v_old, grad_val, clip_factor, learn_rate):
    grad_clip = clip_factor * grad_val
    m_new = BETA_ONE * m_old + (1.0 - BETA_ONE) * grad_clip
    v_new = BETA_TWO * v_old + (1.0 - BETA_TWO) * grad_clip * grad_clip
    m_hat = m_new / (1.0 - BETA_ONE ** ADAM_STEP)
    v_hat = v_new / (1.0 - BETA_TWO ** ADAM_STEP)
    w_new = w_old - learn_rate * (m_hat / (jnp.sqrt(v_hat) + ADAM_EPS) + WEIGHT_DECAY * w_old)
    return w_new, m_new, v_new


def solution(mesh):
    n_stage = mesh.shape["stage"]
    n_data = mesh.shape["data"]

    def device_step(x_loc, t_loc, w1_loc, w2_loc, wm_loc, m_loc, v_loc):
        n_micro, n_tok, d_model = x_loc.shape
        n_blk, d_ff = w1_loc.shape[2], w1_loc.shape[4]
        n_tokens = n_micro * n_tok * n_data
        n_blocks = 2 * n_stage * n_blk
        tau_clip = 0.3 * d_model * math.sqrt(n_blocks * (3.0 / n_tokens + 0.008))
        learn_rate = 0.1 / math.sqrt(4.0 * d_model * n_blocks)
        rows = n_micro * n_tok // n_stage
        w1 = lax.all_gather(w1_loc, "stage", axis=0, tiled=True).reshape(n_blocks, d_model, d_ff)
        w2 = lax.all_gather(w2_loc, "stage", axis=0, tiled=True).reshape(n_blocks, d_ff, d_model)
        off = (lax.axis_index("stage") * (rows // (2 * ROWS))).astype(jnp.int32).reshape(1)
        g1, g2, loss = run_stack(x_loc.reshape(-1, d_model), t_loc.reshape(-1, d_model), w1, w2, off, rows, n_tokens)
        g2 = jnp.swapaxes(g2, 1, 2)
        flat = jnp.concatenate([g1.reshape(n_stage, 2, n_blk, -1), g2.reshape(n_stage, 2, n_blk, -1)], axis=-1)
        mine = lax.psum_scatter(flat, "stage", scatter_dimension=0, tiled=True)
        grad_shard = lax.psum_scatter(mine, "data", scatter_dimension=3, tiled=True)[0]
        sums = lax.psum(jnp.stack([jnp.sum(grad_shard * grad_shard), 0.5 * jnp.sum(loss)]), ("stage", "data"))
        clip_factor = jnp.minimum(1.0, tau_clip / jnp.sqrt(sums[0]))
        w_new, m_new, v_new = adam_update(wm_loc[0], m_loc[0], v_loc[0], grad_shard, clip_factor, learn_rate)
        w_full = lax.all_gather(w_new.astype(jnp.bfloat16), "data", axis=2, tiled=True)
        split_at = d_model * d_ff
        w1_new = w_full[:, :, :split_at].reshape(1, 2, n_blk, d_model, d_ff)
        w2_new = w_full[:, :, split_at:].reshape(1, 2, n_blk, d_ff, d_model)
        return w1_new, w2_new, w_new[None], m_new[None], v_new[None], sums[1] / n_tokens

    act_spec = P(None, "data", None)
    flat_spec = P("stage", None, None, "data")
    return jax.shard_map(device_step, mesh=mesh, in_specs=(act_spec, act_spec, P("stage"), P("stage"), flat_spec, flat_spec, flat_spec), out_specs=(P("stage"), P("stage"), flat_spec, flat_spec, flat_spec, P()), check_vma=False)
```
